32 devices in a mesh: seq: 8 (over z, y), head: 4 (over x, core).
Axes of the slice: x: 2, y: 2, z: 4, core: 2. Of those that a mesh axis runs over, the one named last changes fastest.
Arguments:
- query_rows: bfloat16 [8192, 4096], P('seq', 'head'), may hold values from -6 to 6
- key_rows: bfloat16 [8192, 4096], P('seq', 'head'), may hold values from -6 to 6
- value_rows: bfloat16 [8192, 4096], P('seq', 'head'), may hold values from -15 to 15
- block_picks: int32 [16, 32, 4], P('seq', 'head'), may hold values from -1 to 15, as said below
- out_weight: bfloat16 [4096, 4096], P(None, 'head'), may hold values from -0.09375 to 0.09375
Outputs:
- mixed: bfloat16 [8192, 4096], P('seq', 'head')
The draws below stay inside these ranges and needn't reach their ends.
Inputs may be any that keep to these rules, and one draw needn't show every extreme that they name: `block_picks`: every entry that is not -1 names a block held by a lower index of seq than block b. Repeated entries of one row count once. Over the query blocks of one index of seq and the heads of one index of head, at most 2 entries name blocks of any one other index of seq, and every index of seq from 1 on has exactly 2 entries naming blocks of index 0.
All inputs are finite; a program needn't handle non-finite values.
Results may differ from the reference program's by a relative error of at most 0.0059.
Values may be sent and summed in bfloat16 or wider, within the bound.
A program may use at most 192 MiB of HBM per device.

```python
import jax
import jax.numpy as jnp
import numpy as np
from jax import lax

HEADS = 32
HEAD_DIM = 128
D = 4096
BLOCK = 512
TOPK = 5
CAP = 2
BLK_DEV = 2
SEQ = 8192
N_SEQ = 8
N_HEAD = 4


def drawn_pair(key):
    row_count = BLK_DEV * BLOCK * N_SEQ
    width_all = HEADS * HEAD_DIM
    streams = jax.random.split(jax.random.fold_in(key, 7001), 2)
    queries = jnp.clip(1.5 * jax.random.normal(streams[0], (row_count, width_all), jnp.float32), -6.0, 6.0)
    keys_drawn = jnp.clip(1.5 * jax.random.normal(streams[1], (row_count, width_all), jnp.float32), -6.0, 6.0)
    return (queries, keys_drawn)


def draw_query_rows(key, part):
    return drawn_pair(key)[0].astype(jnp.bfloat16)


def draw_key_rows(key, part):
    return drawn_pair(key)[1].astype(jnp.bfloat16)


def draw_block_picks(key, part):
    group_heads = HEADS // N_HEAD
    pair_count = BLK_DEV * group_heads
    slot_count = TOPK - 1
    entry_count = pair_count * slot_count
    seat_count = (N_SEQ - 1) * CAP
    later_count = entry_count - CAP
    later_entries = jnp.asarray(np.array([index_value for index_value in range(entry_count) if index_value % slot_count != 0], dtype=np.int32))

    def one_list(group_id, requester):
        list_key = jax.random.fold_in(jax.random.fold_in(key, 9103), group_id * N_SEQ + requester)
        streams = jax.random.split(list_key, 4)
        first_entries = jax.random.permutation(streams[0], pair_count).astype(jnp.int32) * slot_count
        later_order = jax.random.permutation(streams[1], later_entries).astype(jnp.int32)
        order_list = jnp.concatenate([first_entries, later_order])
        seat_perm = jax.random.permutation(streams[2], seat_count).astype(jnp.int32)
        seat_owner = seat_perm // CAP + 1
        blocked = (seat_owner >= requester).astype(jnp.int32)
        ranked = jnp.argsort(blocked * seat_count + jnp.arange(seat_count, dtype=jnp.int32))
        usable_count = jnp.sum(1 - blocked)
        sorted_owner = jnp.concatenate([seat_owner[ranked], jnp.full((later_count,), -1, jnp.int32)])
        position = jnp.arange(later_count, dtype=jnp.int32)
        later_owner = jnp.where(position < usable_count, sorted_owner[position], -1)
        hot_owner = jnp.where(requester >= 1, jnp.zeros((CAP,), jnp.int32), -1)
        owners = jnp.concatenate([hot_owner, later_owner])
        within = jax.random.randint(streams[3], (entry_count,), 0, BLK_DEV).astype(jnp.int32)
        chosen = jnp.where(owners >= 0, owners * BLK_DEV + within, -1)
        listed = jnp.zeros((entry_count,), jnp.int32).at[order_list].set(chosen)
        return listed.reshape(BLK_DEV, group_heads, slot_count)
    requesters = jnp.arange(N_SEQ, dtype=jnp.int32)
    all_lists = jax.vmap(lambda group_id: jax.vmap(lambda requester: one_list(group_id, requester))(requesters))(jnp.arange(N_HEAD, dtype=jnp.int32))
    all_lists = jnp.transpose(all_lists, (1, 2, 0, 3, 4))
    return all_lists.reshape(N_SEQ * BLK_DEV, HEADS, slot_count)


def block_scale(stream_key, extent, pieces, smallest, high):
    def one(axis_at, shards_of):
        draws = jax.random.uniform(jax.random.fold_in(jax.random.fold_in(stream_key, 6), axis_at), (shards_of,), jnp.float32, smallest / len(pieces), high / len(pieces))
        return jnp.repeat(jnp.exp(draws), extent[axis_at] // shards_of).reshape((-1,) + (1,) * (len(extent) - axis_at - 1))

    factor_of = one(*pieces[0])
    for cut in pieces[1:]:
        factor_of = factor_of * one(*cut)
    return factor_of


def gaussian(rng, dims, deviation, bound, shards=(), held_as=jnp.bfloat16):
    drawn = deviation * jax.random.normal(rng, dims, jnp.float32)
    if shards:
        drawn = drawn * block_scale(rng, dims, shards, -0.22, 0.18)
    return jnp.clip(drawn, -bound, bound).astype(held_as)


def setup_inputs(seed: int = 0) -> dict:
    key_of = jax.random.split(jax.random.key(seed), 6)
    query_rows = draw_query_rows(jax.random.fold_in(key_of[5], 71), 0)
    key_rows = draw_key_rows(jax.random.fold_in(key_of[5], 71), 0)
    value_rows = gaussian(key_of[2], (SEQ, HEADS * HEAD_DIM), 3.0, 15.0, ((0, 8), (1, 4)))
    block_picks = draw_block_picks(jax.random.fold_in(key_of[5], 71), 0)
    out_weight = gaussian(key_of[4], (HEADS * HEAD_DIM, D), (HEADS * HEAD_DIM) ** -0.5, 0.09375, ((1, 4),))
    return {"query_rows": query_rows, "key_rows": key_rows, "value_rows": value_rows, "block_picks": block_picks, "out_weight": out_weight}


def block_partial(query_tile, key_tile, value_tile, causal_mask):
    score_scale = HEAD_DIM ** -0.5
    scores = jnp.einsum("hqd,hkd->hqk", query_tile.astype(jnp.float32), key_tile.astype(jnp.float32)) * score_scale
    if causal_mask is not None:
        scores = jnp.where(causal_mask, scores, -jnp.inf)
    maxima = jnp.max(scores, axis=-1)
    shifted = jnp.exp(scores - maxima[..., None])
    totals = jnp.sum(shifted, axis=-1)
    weights = shifted.astype(jnp.bfloat16)
    partial_out = jnp.einsum("hqk,hkd->hqd", weights.astype(jnp.float32), value_tile.astype(jnp.float32))
    return partial_out.astype(jnp.bfloat16), maxima, totals


def merge_parts(outputs, maxima, totals, usable):
    keep = usable[:, :, None]
    largest = jnp.max(jnp.where(keep, maxima, -jnp.inf), axis=0)
    factor = jnp.where(keep, jnp.exp(maxima - largest[None]), 0.0)
    numer = jnp.sum(factor[..., None] * outputs.astype(jnp.float32), axis=0)
    denom = jnp.sum(factor * totals, axis=0)
    return (numer / denom[..., None]).astype(jnp.bfloat16)


def reference(query_rows, key_rows, value_rows, block_picks, out_weight):
    block_count = query_rows.shape[0] // BLOCK
    block_shape = (block_count, BLOCK, HEADS, HEAD_DIM)
    queries = query_rows.reshape(block_shape)
    key_blocks = key_rows.reshape(block_shape)
    value_blocks = value_rows.reshape(block_shape)
    positions = jnp.arange(BLOCK)
    causal_mask = positions[:, None] >= positions[None, :]
    head_index = jnp.arange(HEADS)

    def one_block(block_id):
        query_tile = jnp.transpose(queries[block_id], (1, 0, 2))
        own_part = block_partial(query_tile, jnp.transpose(key_blocks[block_id], (1, 0, 2)),
                                 jnp.transpose(value_blocks[block_id], (1, 0, 2)), causal_mask)
        chosen = block_picks[block_id]
        part_outputs = [own_part[0]]
        part_maxima = [own_part[1]]
        part_totals = [own_part[2]]
        part_usable = [jnp.ones((HEADS,), dtype=jnp.bool_)]
        for column in range(chosen.shape[1]):
            entries = chosen[:, column]
            usable = entries >= 0
            for earlier in range(column):
                usable = usable & (entries != chosen[:, earlier])
            safe_index = jnp.where(usable, entries, 0)
            result_part = block_partial(query_tile, key_blocks[safe_index, :, head_index, :],
                                        value_blocks[safe_index, :, head_index, :], None)
            part_outputs.append(result_part[0])
            part_maxima.append(result_part[1])
            part_totals.append(result_part[2])
            part_usable.append(usable)
        combined = merge_parts(jnp.stack(part_outputs), jnp.stack(part_maxima), jnp.stack(part_totals),
                               jnp.stack(part_usable))
        return jnp.transpose(combined, (1, 0, 2)).reshape(BLOCK, HEADS * HEAD_DIM)

    attended = lax.map(one_block, jnp.arange(block_count, dtype=jnp.int32)).reshape(-1, HEADS * HEAD_DIM)
    return jnp.dot(attended, out_weight, preferred_element_type=jnp.float32).astype(jnp.bfloat16)
```

```python
import functools
import math

import jax
import jax.numpy as jnp
from jax import lax
from jax.experimental import pallas as pl
from jax.experimental.pallas import tpu as pltpu
from jax.sharding import PartitionSpec as P

CAP = 2
MESH = pl.DeviceIdType.MESH
F32 = jnp.float32
BF16 = jnp.bfloat16


def loop(lower, upper, step):
    def body(i, carry):
        step(i)
        return carry

    lax.fori_loop(lower, upper, body, 0)


def attend(query, key, value, causal_start=None):
    scale = query.shape[-1] ** -0.5
    scores = lax.dot_general(
        key, query, (((1,), (1,)), ((), ())), preferred_element_type=F32
    )
    if causal_start is not None:
        key_at = lax.broadcasted_iota(jnp.int32, scores.shape, 0)
        query_at = lax.broadcasted_iota(jnp.int32, scores.shape, 1) + causal_start
        scores = jnp.where(key_at <= query_at, scores, -jnp.inf)
    top = jnp.max(scores, axis=0, keepdims=True)
    weights = jnp.exp2((scores - top) * (scale * math.log2(math.e)))
    total = jnp.sum(weights, axis=0, keepdims=True)
    part = lax.dot_general(
        value, weights.astype(BF16), (((0,), (0,)), ((), ())), preferred_element_type=F32
    )
    return part / total, top * scale + jnp.log(total)


def kernel(
    dims,
    q_hbm,
    k_hbm,
    v_hbm,
    picks,
    w_hbm,
    out,
    q,
    k,
    v,
    w,
    owner,
    first,
    tile_at,
    ask,
    asking,
    asked,
    order,
    orders,
    q_out,
    q_in,
    o_out,
    o_in,
    l_out,
    l_in,
    o_all,
    l_all,
    own_g,
    mate_g,
    cross_g,
    fwd_g,
    acc,
    load_sem,
    w_sem,
    ask_sem,
    order_sem,
    q_sem,
    o_sem,
    l_sem,
    near_sem,
    cross_sem,
    fwd_sem,
):
    n_seq, n_head, blocks, heads, n_pick, rows, width = dims
    pairs = blocks * heads
    n_x = n_head // 2
    me = lax.axis_index("seq")
    hd = lax.axis_index("head")
    hx, hc = lax.div(hd, 2), lax.rem(hd, 2)
    mate = hx * 2 + 1 - hc
    half = rows // 2
    n_tiles = me * CAP
    n_serve = (n_seq - 1 - me) * CAP
    free = jnp.maximum(pairs - n_tiles, 0)
    odd = lax.rem(me, 2)
    lines, line = n_seq // 2, lax.div(me, 2)
    middle = lines // 2

    def across(step):
        return lax.rem(hx + step, n_x) * 2 + hc

    def behind(step):
        return lax.rem(hx + n_x - step, n_x) * 2 + hc

    def load(i, p):
        src, dst = ((q_hbm, q), (k_hbm, k), (v_hbm, v))[i]
        b, h = lax.div(p, heads), lax.rem(p, heads)
        return pltpu.make_async_copy(
            src.at[
                pl.ds(pl.multiple_of(b * rows, rows), rows),
                pl.ds(pl.multiple_of(h * width, width), width),
            ],
            dst.at[p],
            load_sem.at[i, p],
        )

    weight_load = pltpu.make_async_copy(w_hbm, w, w_sem.at[0])
    loop(0, pairs, lambda p: load(0, p).start())

    barrier = pltpu.get_barrier_semaphore()

    def greet(d):
        pl.semaphore_signal(
            barrier, inc=1, device_id={"seq": lax.rem(me + d, n_seq)}, device_id_type=MESH
        )

    loop(1, n_seq, greet)
    for d in range(1, n_head):
        pl.semaphore_signal(
            barrier, inc=1, device_id={"head": lax.rem(hd + d, n_head)}, device_id_type=MESH
        )

    for i in range(1, 3):
        loop(0, pairs, lambda p, i=i: load(i, p).start())

    def find_owner(p):
        b, h = lax.div(p, heads), lax.rem(p, heads)
        found = [picks[b, t, h] for t in range(n_pick)]
        for t in range(n_pick):
            fresh = found[t] >= 0
            for earlier in range(t):
                fresh = fresh & (found[t] != found[earlier])
            owner[p * n_pick + t] = jnp.where(fresh, lax.div(found[t], blocks), -1)

    loop(0, pairs, find_owner)

    def clear(s):
        first[s] = 0

    loop(0, n_seq, clear)

    def find_asks(d):
        s = me - 1 - d

        def scan(p, carry):
            low, high = carry
            for t in range(n_pick):
                e = p * n_pick + t
                hit = owner[e] == s
                low = jnp.minimum(low, jnp.where(hit, e, pairs * n_pick))
                high = jnp.maximum(high, jnp.where(hit, e, 0))
            return low, high

        low, high = lax.fori_loop(0, pairs, scan, (jnp.int32(pairs * n_pick), jnp.int32(0)))
        first[s] = low
        for c, e in enumerate((jnp.where(low < pairs * n_pick, low, 0), high)):
            p = lax.div(e, n_pick)
            b, h = lax.div(p, heads), lax.rem(p, heads)
            pick = jnp.maximum(picks[b, lax.rem(e, n_pick), h], 0)
            ask[s, c] = lax.rem(pick, blocks) * heads + h
            asking[s, c] = p

    def ask_copy(s, r):
        return pltpu.make_async_remote_copy(
            src_ref=ask.at[s],
            dst_ref=asked.at[r],
            send_sem=ask_sem.at[0, s],
            recv_sem=ask_sem.at[1, r],
            device_id={"seq": s},
            device_id_type=MESH,
        )

    def tile_copy(source, landing, sems, there, here, target):
        return pltpu.make_async_remote_copy(
            src_ref=source.at[there],
            dst_ref=landing.at[here],
            send_sem=sems.at[0, there],
            recv_sem=sems.at[1, here],
            device_id={"seq": target},
            device_id_type=MESH,
        )

    def q_copy(s, r, c):
        return tile_copy(q_out, q_in, q_sem, s * CAP + c, r * CAP + c, s)

    def o_copy(r, s, c):
        return tile_copy(o_out, o_in, o_sem, r * CAP + c, s * CAP + c, r)

    def l_copy(r, s, c):
        return tile_copy(l_out, l_in, l_sem, r * CAP + c, s * CAP + c, r)

    def at_least(value, bound):
        return lax.div(value - bound + 4 * n_seq, 4 * n_seq)

    def pick(flag, yes, no):
        return flag * yes + (1 - flag) * no

    def source_of(n):
        lone = odd * CAP
        is_late = at_least(n, lone)
        late = (n - lone) * is_late
        group = lax.div(late, 2 * CAP)
        there = pick(downward, line - 1 - group, group)
        s = 2 * there + 1 - lax.rem(late, 2)
        c = lax.div(lax.rem(late, 2 * CAP), 2)
        return pick(is_late, s, me - 1), pick(is_late, c, n)

    def tile_of(s, c):
        there = lax.div(s, 2)
        group = pick(downward, line - 1 - there, there)
        late = odd * CAP + group * (2 * CAP) + c * 2 + 1 - lax.rem(s, 2)
        return jnp.where(there == line, c, late)

    downward = at_least(line, middle + 1)
    beyond = pick(downward, line, middle) + 1
    n_near = lines - beyond

    def requester_of(n):
        lone = (1 - odd) * CAP
        is_late = at_least(n, lone)
        late = (n - lone) * is_late
        group = lax.div(late, 2 * CAP)
        low = pick(at_least(group, middle), group + 1, middle - group)
        high = pick(at_least(group, n_near), line + 1 + group - n_near, beyond + group)
        r = 2 * pick(at_least(line, 1), high, low) + lax.rem(late, 2)
        c = lax.div(lax.rem(late, 2 * CAP), 2)
        return pick(is_late, r, me + 1), pick(is_late, c, n)

    def start_rows(b):
        acc[b] = jnp.zeros(acc.shape[1:], F32)

    loop(0, me, find_asks)
    loop(0, blocks, start_rows)
    loop(0, pairs, lambda p: load(0, p).wait())

    def stage(n):
        s, c = source_of(n)
        q_out[s * CAP + c] = q[asking[s, c]]

    def send(n):
        s, c = source_of(n)

        @pl.when(c == 0)
        def _():
            ask_copy(s, me).start()

        q_copy(s, me, c).start()

    loop(0, n_tiles, stage)
    pl.semaphore_wait(barrier, n_seq + n_head - 2)
    loop(0, n_tiles, send)

    def place(p):
        key = jnp.int32(-1)
        for t in range(n_pick):
            e = p * n_pick + t
            s = owner[e]
            c = jnp.where(first[jnp.maximum(s, 0)] == e, 0, 1)
            at = jnp.where(s >= 0, tile_of(s, c), -1)
            tile_at[e] = at
            key = jnp.maximum(key, at)
        owner[p * n_pick] = key * pairs + p

    loop(0, pairs, place)

    def rank(p):
        key = owner[p * n_pick]
        ahead = jnp.int32(0)
        for other in range(pairs):
            ahead = ahead + jnp.where(owner[other * n_pick] < key, 1, 0)
        order[1, p] = ahead

    loop(0, pairs, rank)

    def invert(i):
        found = jnp.int32(0)
        for p in range(pairs):
            found = found + jnp.where(order[1, p] == i, p, 0)
        order[0, i] = found

    loop(0, pairs, invert)

    def order_copy(d):
        target = lax.rem(hd + d, n_head)
        return pltpu.make_async_remote_copy(
            src_ref=order,
            dst_ref=orders.at[hd],
            send_sem=order_sem.at[0, d],
            recv_sem=order_sem.at[1, hd],
            device_id={"head": target},
            device_id_type=MESH,
        )

    def order_wait(d):
        source = lax.rem(hd + d, n_head)
        return pltpu.make_async_remote_copy(
            src_ref=order,
            dst_ref=orders.at[source],
            send_sem=order_sem.at[0, d],
            recv_sem=order_sem.at[1, source],
            device_id={"head": source},
            device_id_type=MESH,
        )

    for d in range(1, n_head):
        order_copy(d).start()

    for i in range(1, 3):
        loop(0, pairs, lambda p, i=i: load(i, p).wait())
    weight_load.start()

    def head_copy(src, dst, sems, target):
        return pltpu.make_async_remote_copy(
            src_ref=src,
            dst_ref=dst,
            send_sem=sems[0],
            recv_sem=sems[1],
            device_id={"head": target},
            device_id_type=MESH,
        )

    def near_copy(i):
        sems = (near_sem.at[0, i], near_sem.at[1, i])
        return head_copy(own_g.at[i], mate_g.at[i], sems, mate)

    def cross_copy(step, i):
        sems = (cross_sem.at[0, step - 1, i], cross_sem.at[1, step - 1, i])
        return head_copy(own_g.at[i], cross_g.at[step - 1, i], sems, across(step))

    def fwd_copy(step, i):
        sems = (fwd_sem.at[0, step - 1, i], fwd_sem.at[1, step - 1, i])
        return head_copy(cross_g.at[step - 1, i], fwd_g.at[step - 1, i], sems, mate)

    def merge(p, span, part, level):
        levels, tiles = [], []
        for t in range(n_pick):
            at = tile_at[p * n_pick + t]
            safe = jnp.maximum(at, 0)
            levels.append(jnp.where(at >= 0, l_all[safe, :, span], -jnp.inf))
            tiles.append((at, safe))
        largest = level
        for far in levels:
            largest = jnp.maximum(largest, far)
        factor = jnp.exp(level - largest)
        denom = factor
        factors = []
        for far in levels:
            factors.append(jnp.exp(far - largest))
            denom = denom + factors[-1]
        numer = (factor / denom) * part
        for (at, safe), far in zip(tiles, factors):
            far_part = o_all[safe, :, span].astype(F32)
            numer = numer + jnp.where(at >= 0, (far / denom) * far_part, 0.0)
        return numer

    def position(i, gated):
        p = order[0, i]
        query, key, value = q[p], k[p], v[p]
        for part in range(2):
            seen = (part + 1) * half
            span = slice(part * half, seen)
            result, level = attend(query[span], key[:seen], value[:seen], part * half)
            if gated:
                result = merge(p, span, result, level)
            own_g[i, span, :] = result.T.astype(BF16)
        for step in range(1, n_x):
            cross_copy(step, i).start()
        near_copy(i).start()

    def serve(n):
        r, c = requester_of(n)
        slot = r * CAP + c

        @pl.when(c == 0)
        def _():
            ask_copy(me, r).wait_recv()

        q_copy(me, r, c).wait_recv()
        code = asked[r, c]
        query, key, value = q_in[slot], k[code], v[code]
        for part in range(2):
            span = slice(part * half, (part + 1) * half)
            result, level = attend(query[span], key, value)
            o_out[slot, :, span] = result.astype(BF16)
            l_out[slot, :, span] = level
        l_copy(r, me, c).start()
        o_copy(r, me, c).start()

    def take_tile(n):
        s, c = source_of(n)
        l_copy(s, s, c).wait_recv()
        o_copy(s, s, c).wait_recv()
        o_all[n] = o_in[s * CAP + c]
        l_all[n] = l_in[s * CAP + c]

    def forward(i):
        for step in range(1, n_x):
            cross_copy(step, i).wait_recv()
            fwd_copy(step, i).start()

    def project(sources, places, tiles):
        weights = jnp.concatenate(
            [
                w[source * heads + lax.rem(p, heads)]
                for source, p in zip(sources, places)
            ],
            axis=0,
        )
        for b in range(blocks):
            seen = jnp.concatenate(
                [
                    jnp.where(lax.div(p, heads) == b, tile, jnp.zeros_like(tile))
                    for p, tile in zip(places, tiles)
                ],
                axis=1,
            )
            acc[b] += jnp.dot(seen, weights, preferred_element_type=F32)

    def project_near(i):
        near_copy(i).wait_recv()
        project((hd, mate), (order[0, i], orders[mate, 0, i]), (own_g[i], mate_g[i]))

    def project_far(i):
        for step in range(1, n_x):
            fwd_copy(step, i).wait_recv()
            from_x = behind(step)
            from_mate = lax.rem(hx + n_x - step, n_x) * 2 + 1 - hc
            project(
                (from_x, from_mate),
                (orders[from_x, 0, i], orders[from_mate, 0, i]),
                (cross_g[step - 1, i], fwd_g[step - 1, i]),
            )

    def pass_on(i):
        forward(i)
        project_near(i)

        @pl.when(i > 0)
        def _():
            project_far(i - 1)

    loop(0, free, lambda i: position(i, False))
    weight_load.wait()
    for d in range(1, n_head):
        order_wait(d).wait_recv()

    n_late = jnp.where(line > 0, jnp.maximum(middle - line, 0) * 2 * CAP, 0)
    n_soon = n_serve - n_late
    ready = jnp.maximum(free - 1, 0)

    def passed(n):
        return jnp.clip(n - 1 - me, 0, ready)

    def soon_step(n):
        serve(n)
        loop(passed(n - 1), passed(n), pass_on)

    loop(0, n_soon, soon_step)
    start = passed(n_soon - 1)

    def gate(i):
        return jnp.maximum(n_tiles - (pairs - 1 - i), 0)

    def passed_gated(i):
        return jnp.where((n_late > 0) | (i < free), start, jnp.maximum(i - 1, start))

    def gated_step(i):
        loop(jnp.where(i == free, 0, gate(i - 1)), gate(i), take_tile)
        position(i, True)
        loop(passed_gated(i - 1), passed_gated(i), pass_on)

    loop(free, pairs, gated_step)
    middle_pass = passed_gated(jnp.where(free < pairs, pairs - 1, free - 1))

    def passed_late(n):
        here = jnp.maximum(pairs - 3 - n_serve + n, middle_pass)
        return jnp.where(n < n_soon, middle_pass, jnp.clip(here, 0, pairs - 1))

    def late_step(n):
        loop(passed_late(n - 1), passed_late(n), pass_on)
        serve(n)

    loop(n_soon, n_serve, late_step)
    loop(passed_late(n_serve - 1), pairs - 1, pass_on)
    project_near(pairs - 1)
    forward(pairs - 1)
    loop(pairs - 2, pairs, project_far)

    def finish(b):
        out[pl.ds(pl.multiple_of(b * rows, rows), rows), :] = acc[b].astype(BF16)

    loop(0, blocks, finish)

    def sent_asks(s):
        ask_copy(s, me).wait_send()
        for c in range(CAP):
            q_copy(s, me, c).wait_send()

    loop(0, me, sent_asks)

    def sent_results(r):
        for c in range(CAP):
            o_copy(r, me, c).wait_send()
            l_copy(r, me, c).wait_send()

    loop(me + 1, n_seq, sent_results)
    for d in range(1, n_head):
        order_copy(d).wait_send()

    def sent_heads(i):
        near_copy(i).wait_send()
        for step in range(1, n_x):
            cross_copy(step, i).wait_send()
            fwd_copy(step, i).wait_send()

    loop(0, pairs, sent_heads)


def solution(mesh):
    n_seq, n_head = mesh.shape["seq"], mesh.shape["head"]

    def body(query_rows, key_rows, value_rows, block_picks, out_weight):
        tok_rows, feature_width = query_rows.shape
        blocks, heads, n_pick = block_picks.shape
        rows, width = tok_rows // blocks, feature_width // heads
        pairs = blocks * heads
        crossings = max(n_head // 2 - 1, 1)
        any_spec = pl.BlockSpec(memory_space=pl.ANY)
        smem_spec = pl.BlockSpec(memory_space=pltpu.SMEM)
        vmem_spec = pl.BlockSpec(memory_space=pltpu.VMEM)
        out_width = out_weight.shape[1]
        slots = n_seq * CAP
        dma = pltpu.SemaphoreType.DMA
        dims = (n_seq, n_head, blocks, heads, n_pick, rows, width)
        tiles = pltpu.VMEM((pairs, rows, width), BF16)
        return pl.pallas_call(
            functools.partial(kernel, dims),
            out_shape=jax.ShapeDtypeStruct((tok_rows, out_width), BF16),
            in_specs=[any_spec] * 3 + [smem_spec] + [any_spec],
            out_specs=vmem_spec,
            scratch_shapes=[
                tiles,
                tiles,
                tiles,
                pltpu.VMEM((out_weight.shape[0] // width, width, out_width), BF16),
                pltpu.SMEM((pairs * n_pick,), jnp.int32),
                pltpu.SMEM((n_seq,), jnp.int32),
                pltpu.SMEM((pairs * n_pick,), jnp.int32),
                pltpu.SMEM((n_seq, CAP), jnp.int32),
                pltpu.SMEM((n_seq, CAP), jnp.int32),
                pltpu.SMEM((n_seq, CAP), jnp.int32),
                pltpu.SMEM((2, pairs), jnp.int32),
                pltpu.SMEM((n_head, 2, pairs), jnp.int32),
                pltpu.VMEM((slots, rows, width), BF16),
                pltpu.VMEM((slots, rows, width), BF16),
                pltpu.VMEM((slots, width, rows), BF16),
                pltpu.VMEM((slots, width, rows), BF16),
                pltpu.VMEM((slots, 1, rows), F32),
                pltpu.VMEM((slots, 1, rows), F32),
                pltpu.VMEM((slots, width, rows), BF16),
                pltpu.VMEM((slots, 1, rows), F32),
                tiles,
                tiles,
                pltpu.VMEM((crossings, pairs, rows, width), BF16),
                pltpu.VMEM((crossings, pairs, rows, width), BF16),
                pltpu.VMEM((blocks, rows, out_width), F32),
                dma((3, pairs)),
                dma((1,)),
                dma((2, n_seq)),
                dma((2, n_head)),
                dma((2, slots)),
                dma((2, slots)),
                dma((2, slots)),
                dma((2, pairs)),
                dma((2, crossings, pairs)),
                dma((2, crossings, pairs)),
            ],
            compiler_params=pltpu.CompilerParams(
                collective_id=0,
                has_side_effects=True,
                vmem_limit_bytes=67043328,
            ),
            name="layer",
        )(query_rows, key_rows, value_rows, jnp.swapaxes(block_picks, 1, 2),
          out_weight.reshape(-1, width, out_width))

    return jax.shard_map(
        body,
        mesh=mesh,
        in_specs=(
            P("seq", "head"),
            P("seq", "head"),
            P("seq", "head"),
            P("seq", "head", None),
            P(None, "head"),
        ),
        out_specs=P("seq", "head"),
        check_vma=False,
    )
```

```python
import functools
import math

import jax
import jax.numpy as jnp
from jax import lax
from jax.experimental import pallas as pl
from jax.experimental.pallas import tpu as pltpu
from jax.sharding import PartitionSpec as P

CAP = 2
MESH = pl.DeviceIdType.MESH
F32 = jnp.float32
BF16 = jnp.bfloat16


def loop(lower, upper, step):
    def body(i, carry):
        step(i)
        return carry

    lax.fori_loop(lower, upper, body, 0)


def attend(query, key, value, causal_start=None):
    scale = query.shape[-1] ** -0.5
    scores = lax.dot_general(
        key, query, (((1,), (1,)), ((), ())), preferred_element_type=F32
    )
    if causal_start is not None:
        key_at = lax.broadcasted_iota(jnp.int32, scores.shape, 0)
        query_at = lax.broadcasted_iota(jnp.int32, scores.shape, 1) + causal_start
        scores = jnp.where(key_at <= query_at, scores, -jnp.inf)
    top = jnp.max(scores, axis=0, keepdims=True)
    weights = jnp.exp2((scores - top) * (scale * math.log2(math.e)))
    total = jnp.sum(weights, axis=0, keepdims=True)
    part = lax.dot_general(
        value, weights.astype(BF16), (((0,), (0,)), ((), ())), preferred_element_type=F32
    )
    return part / total, top * scale + jnp.log(total)


def kernel(
    dims,
    q_hbm,
    k_hbm,
    v_hbm,
    picks,
    w_hbm,
    out,
    q,
    k,
    v,
    w,
    owner,
    first,
    tile_at,
    ask,
    asking,
    asked,
    order,
    orders,
    q_out,
    q_in,
    o_out,
    o_in,
    l_out,
    l_in,
    o_all,
    l_all,
    own_g,
    mate_g,
    cross_g,
    fwd_g,
    acc,
    load_sem,
    w_sem,
    ask_sem,
    order_sem,
    q_sem,
    o_sem,
    l_sem,
    near_sem,
    cross_sem,
    fwd_sem,
):
    n_seq, n_head, blocks, heads, n_pick, rows, width = dims
    pairs = blocks * heads
    n_x = n_head // 2
    me = lax.axis_index("seq")
    hd = lax.axis_index("head")
    hx, hc = lax.div(hd, 2), lax.rem(hd, 2)
    mate = hx * 2 + 1 - hc
    half = rows // 2
    n_tiles = me * CAP
    n_serve = (n_seq - 1 - me) * CAP
    free = jnp.maximum(pairs - n_tiles, 0)
    odd = lax.rem(me, 2)
    lines, line = n_seq // 2, lax.div(me, 2)
    middle = lines // 2

    def across(step):
        return lax.rem(hx + step, n_x) * 2 + hc

    def behind(step):
        return lax.rem(hx + n_x - step, n_x) * 2 + hc

    def load(i, p):
        src, dst = ((q_hbm, q), (k_hbm, k), (v_hbm, v))[i]
        b, h = lax.div(p, heads), lax.rem(p, heads)
        return pltpu.make_async_copy(
            src.at[
                pl.ds(pl.multiple_of(b * rows, rows), rows),
                pl.ds(pl.multiple_of(h * width, width), width),
            ],
            dst.at[p],
            load_sem.at[i, p],
        )

    weight_load = pltpu.make_async_copy(w_hbm, w, w_sem.at[0])
    loop(0, pairs, lambda p: load(0, p).start())

    barrier = pltpu.get_barrier_semaphore()

    def greet(d):
        pl.semaphore_signal(
            barrier, inc=1, device_id={"seq": lax.rem(me + d, n_seq)}, device_id_type=MESH
        )

    loop(1, n_seq, greet)
    for d in range(1, n_head):
        pl.semaphore_signal(
            barrier, inc=1, device_id={"head": lax.rem(hd + d, n_head)}, device_id_type=MESH
        )

    for i in range(1, 3):
        loop(0, pairs, lambda p, i=i: load(i, p).start())

    def find_owner(p):
        b, h = lax.div(p, heads), lax.rem(p, heads)
        found = [picks[b, t, h] for t in range(n_pick)]
        for t in range(n_pick):
            fresh = found[t] >= 0
            for earlier in range(t):
                fresh = fresh & (found[t] != found[earlier])
            owner[p * n_pick + t] = jnp.where(fresh, lax.div(found[t], blocks), -1)

    loop(0, pairs, find_owner)

    def clear(s):
        first[s] = 0

    loop(0, n_seq, clear)

    def find_asks(d):
        s = me - 1 - d

        def scan(p, carry):
            low, high = carry
            for t in range(n_pick):
                e = p * n_pick + t
                hit = owner[e] == s
                low = jnp.minimum(low, jnp.where(hit, e, pairs * n_pick))
                high = jnp.maximum(high, jnp.where(hit, e, 0))
            return low, high

        low, high = lax.fori_loop(0, pairs, scan, (jnp.int32(pairs * n_pick), jnp.int32(0)))
        first[s] = low
        for c, e in enumerate((jnp.where(low < pairs * n_pick, low, 0), high)):
            p = lax.div(e, n_pick)
            b, h = lax.div(p, heads), lax.rem(p, heads)
            pick = jnp.maximum(picks[b, lax.rem(e, n_pick), h], 0)
            ask[s, c] = lax.rem(pick, blocks) * heads + h
            asking[s, c] = p

    def ask_copy(s, r):
        return pltpu.make_async_remote_copy(
            src_ref=ask.at[s],
            dst_ref=asked.at[r],
            send_sem=ask_sem.at[0, s],
            recv_sem=ask_sem.at[1, r],
            device_id={"seq": s},
            device_id_type=MESH,
        )

    def tile_copy(source, landing, sems, there, here, target):
        return pltpu.make_async_remote_copy(
            src_ref=source.at[there],
            dst_ref=landing.at[here],
            send_sem=sems.at[0, there],
            recv_sem=sems.at[1, here],
            device_id={"seq": target},
            device_id_type=MESH,
        )

    def q_copy(s, r, c):
        return tile_copy(q_out, q_in, q_sem, s * CAP + c, r * CAP + c, s)

    def o_copy(r, s, c):
        return tile_copy(o_out, o_in, o_sem, r * CAP + c, s * CAP + c, r)

    def l_copy(r, s, c):
        return tile_copy(l_out, l_in, l_sem, r * CAP + c, s * CAP + c, r)

    def at_least(value, bound):
        return lax.div(value - bound + 4 * n_seq, 4 * n_seq)

    def pick(flag, yes, no):
        return flag * yes + (1 - flag) * no

    def source_of(n):
        lone = odd * CAP
        is_late = at_least(n, lone)
        late = (n - lone) * is_late
        group = lax.div(late, 2 * CAP)
        there = pick(downward, line - 1 - group, group)
        s = 2 * there + 1 - lax.rem(late, 2)
        c = lax.div(lax.rem(late, 2 * CAP), 2)
        return pick(is_late, s, me - 1), pick(is_late, c, n)

    def tile_of(s, c):
        there = lax.div(s, 2)
        group = pick(downward, line - 1 - there, there)
        late = odd * CAP + group * (2 * CAP) + c * 2 + 1 - lax.rem(s, 2)
        return jnp.where(there == line, c, late)

    downward = at_least(line, middle + 1)
    beyond = pick(downward, line, middle) + 1
    n_near = lines - beyond

    lone_at = 2 * CAP * at_least(lines, line + 2) * at_least(line, middle)

    def requester_of(n):
        past = (1 - odd) * at_least(n, lone_at + CAP)
        is_lone = (1 - odd) * at_least(n, lone_at) - past
        late = (n - past * CAP) * (1 - is_lone)
        group = lax.div(late, 2 * CAP)
        low = pick(at_least(group, middle), group + 1, middle - group)
        high = pick(at_least(group, n_near), line + 1 + group - n_near, beyond + group)
        r = 2 * pick(at_least(line, 1), high, low) + lax.rem(late, 2)
        c = lax.div(lax.rem(late, 2 * CAP), 2)
        return pick(is_lone, me + 1, r), pick(is_lone, n - lone_at, c)

    def start_rows(b):
        acc[b] = jnp.zeros(acc.shape[1:], F32)

    loop(0, me, find_asks)
    loop(0, blocks, start_rows)
    loop(0, pairs, lambda p: load(0, p).wait())

    def stage(n):
        s, c = source_of(n)
        q_out[s * CAP + c] = q[asking[s, c]]

    def send(n):
        s, c = source_of(n)

        @pl.when(c == 0)
        def _():
            ask_copy(s, me).start()

        q_copy(s, me, c).start()

    loop(0, n_tiles, stage)
    pl.semaphore_wait(barrier, n_seq + n_head - 2)
    loop(0, n_tiles, send)

    def place(p):
        key = jnp.int32(-1)
        for t in range(n_pick):
            e = p * n_pick + t
            s = owner[e]
            c = jnp.where(first[jnp.maximum(s, 0)] == e, 0, 1)
            at = jnp.where(s >= 0, tile_of(s, c), -1)
            tile_at[e] = at
            key = jnp.maximum(key, at)
        owner[p * n_pick] = key * pairs + p

    loop(0, pairs, place)

    def rank(p):
        key = owner[p * n_pick]
        ahead = jnp.int32(0)
        for other in range(pairs):
            ahead = ahead + jnp.where(owner[other * n_pick] < key, 1, 0)
        order[1, p] = ahead

    loop(0, pairs, rank)

    def invert(i):
        found = jnp.int32(0)
        for p in range(pairs):
            found = found + jnp.where(order[1, p] == i, p, 0)
        order[0, i] = found

    loop(0, pairs, invert)

    def order_copy(d):
        target = lax.rem(hd + d, n_head)
        return pltpu.make_async_remote_copy(
            src_ref=order,
            dst_ref=orders.at[hd],
            send_sem=order_sem.at[0, d],
            recv_sem=order_sem.at[1, hd],
            device_id={"head": target},
            device_id_type=MESH,
        )

    def order_wait(d):
        source = lax.rem(hd + d, n_head)
        return pltpu.make_async_remote_copy(
            src_ref=order,
            dst_ref=orders.at[source],
            send_sem=order_sem.at[0, d],
            recv_sem=order_sem.at[1, source],
            device_id={"head": source},
            device_id_type=MESH,
        )

    for d in range(1, n_head):
        order_copy(d).start()

    for i in range(1, 3):
        loop(0, pairs, lambda p, i=i: load(i, p).wait())
    weight_load.start()

    def head_copy(src, dst, sems, target):
        return pltpu.make_async_remote_copy(
            src_ref=src,
            dst_ref=dst,
            send_sem=sems[0],
            recv_sem=sems[1],
            device_id={"head": target},
            device_id_type=MESH,
        )

    def near_copy(i):
        sems = (near_sem.at[0, i], near_sem.at[1, i])
        return head_copy(own_g.at[i], mate_g.at[i], sems, mate)

    def cross_copy(step, i):
        sems = (cross_sem.at[0, step - 1, i], cross_sem.at[1, step - 1, i])
        return head_copy(own_g.at[i], cross_g.at[step - 1, i], sems, across(step))

    def fwd_copy(step, i):
        sems = (fwd_sem.at[0, step - 1, i], fwd_sem.at[1, step - 1, i])
        return head_copy(cross_g.at[step - 1, i], fwd_g.at[step - 1, i], sems, mate)

    def merge(p, span, part, level):
        levels, tiles = [], []
        for t in range(n_pick):
            at = tile_at[p * n_pick + t]
            safe = jnp.maximum(at, 0)
            levels.append(jnp.where(at >= 0, l_all[safe, :, span], -jnp.inf))
            tiles.append((at, safe))
        largest = level
        for far in levels:
            largest = jnp.maximum(largest, far)
        factor = jnp.exp(level - largest)
        denom = factor
        factors = []
        for far in levels:
            factors.append(jnp.exp(far - largest))
            denom = denom + factors[-1]
        numer = (factor / denom) * part
        for (at, safe), far in zip(tiles, factors):
            far_part = o_all[safe, :, span].astype(F32)
            numer = numer + jnp.where(at >= 0, (far / denom) * far_part, 0.0)
        return numer

    def position(i, gated):
        p = order[0, i]
        query, key, value = q[p], k[p], v[p]
        for part in range(2):
            seen = (part + 1) * half
            span = slice(part * half, seen)
            result, level = attend(query[span], key[:seen], value[:seen], part * half)
            if gated:
                result = merge(p, span, result, level)
            own_g[i, span, :] = result.T.astype(BF16)
        for step in range(1, n_x):
            cross_copy(step, i).start()
        near_copy(i).start()

    def serve(n):
        r, c = requester_of(n)
        slot = r * CAP + c

        @pl.when(c == 0)
        def _():
            ask_copy(me, r).wait_recv()

        q_copy(me, r, c).wait_recv()
        code = asked[r, c]
        query, key, value = q_in[slot], k[code], v[code]
        for part in range(2):
            span = slice(part * half, (part + 1) * half)
            result, level = attend(query[span], key, value)
            o_out[slot, :, span] = result.astype(BF16)
            l_out[slot, :, span] = level
        l_copy(r, me, c).start()
        o_copy(r, me, c).start()

    def take_tile(n):
        s, c = source_of(n)
        l_copy(s, s, c).wait_recv()
        o_copy(s, s, c).wait_recv()
        o_all[n] = o_in[s * CAP + c]
        l_all[n] = l_in[s * CAP + c]

    def forward(i):
        for step in range(1, n_x):
            cross_copy(step, i).wait_recv()
            fwd_copy(step, i).start()

    def weights_of(source, p):
        return w[source * heads + lax.rem(p, heads)]

    def project(i, sources, buffers):
        places = [orders_of(source, at) for at in (i, i + 1) for source in sources]
        tiles = [buffer(at) for at in (i, i + 1) for buffer in buffers]
        weights = jnp.concatenate(
            [weights_of(source, p) for source, p in zip(sources * 2, places)], axis=0
        )
        for b in range(blocks):
            seen = jnp.concatenate(
                [
                    jnp.where(lax.div(p, heads) == b, tile, jnp.zeros_like(tile))
                    for p, tile in zip(places, tiles)
                ],
                axis=1,
            )
            acc[b] += jnp.dot(seen, weights, preferred_element_type=F32)

    def orders_of(source, at):
        return order[0, at] if source is hd else orders[source, 0, at]

    def project_far(i):
        for step in range(1, n_x):
            from_x = behind(step)
            from_mate = lax.rem(hx + n_x - step, n_x) * 2 + 1 - hc
            fwd_copy(step, i).wait_recv()
            fwd_copy(step, i + 1).wait_recv()
            buffers = (lambda at: cross_g[step - 1, at], lambda at: fwd_g[step - 1, at])
            project(i, (from_x, from_mate), buffers)

    def project_beside(i):
        near_copy(i).wait_recv()
        near_copy(i + 1).wait_recv()
        project(i, (hd, mate), (lambda at: own_g[at], lambda at: mate_g[at]))

    beside = line >= middle

    def project_near(b):
        for tiles, source, where in (
            (own_g, hd, lambda p: order[1, p]),
            (mate_g, mate, lambda p: orders[mate, 1, p]),
        ):
            lined = jnp.concatenate(
                [tiles[where(b * heads + h)] for h in range(heads)], axis=1
            )
            weights = jnp.concatenate([w[source * heads + h] for h in range(heads)], axis=0)
            acc[b] += jnp.dot(lined, weights, preferred_element_type=F32)

    def end_near(i):
        near_copy(i).wait_recv()

    def pass_on(i):
        forward(i)

        @pl.when((i > 0) & (lax.rem(i, 2) == 0))
        def _():
            project_far(i - 2)

        @pl.when((i > 0) & (lax.rem(i, 2) == 0) & beside)
        def _():
            project_beside(i - 2)

    early = jnp.where(line == 0, 4, jnp.where(line < middle, pairs, 2))

    def placed(n):
        return jnp.minimum(free, early + n + 1)

    def free_step(i):
        position(i, False)

    loop(0, placed(-1), free_step)
    weight_load.wait()
    for d in range(1, n_head):
        order_wait(d).wait_recv()

    n_late = jnp.where(line > 0, jnp.maximum(middle - line, 0), lines - 1 - middle) * 2 * CAP
    n_soon = n_serve - n_late
    ready = jnp.maximum(free - 1, 0)

    def passed(n):
        return jnp.clip(n - 1 - me, 0, ready)

    def soon_step(n):
        serve(n)
        loop(placed(n - 1), placed(n), free_step)
        loop(passed(n - 1), passed(n), pass_on)

    loop(0, n_soon, soon_step)
    loop(placed(n_soon - 1), free, free_step)
    start = passed(n_soon - 1)

    def gate(i):
        return jnp.maximum(n_tiles - (pairs - 1 - i), 0)

    def passed_gated(i):
        return jnp.where(i < free, start, jnp.maximum(i - jnp.where(n_late > 0, 6, 2), start))

    def gated_step(i):
        loop(jnp.where(i == free, 0, gate(i - 1)), gate(i), take_tile)
        position(i, True)
        loop(passed_gated(i - 1), passed_gated(i), pass_on)

    loop(free, pairs, gated_step)
    middle_pass = passed_gated(jnp.where(free < pairs, pairs - 1, free - 1))

    def passed_late(n):
        here = jnp.maximum(pairs - 3 - n_serve + n, middle_pass)
        return jnp.where(n < n_soon, middle_pass, jnp.clip(here, 0, pairs - 1))

    def late_step(n):
        loop(passed_late(n - 1), passed_late(n), pass_on)
        serve(n)

    loop(n_soon, n_serve, late_step)
    loop(passed_late(n_serve - 1), pairs - 1, pass_on)
    loop(jnp.where(beside, pairs, 0), pairs, end_near)

    @pl.when(beside)
    def _():
        project_beside(pairs - 2)

    def last_steps(b):
        @pl.when(jnp.logical_not(beside))
        def _():
            project_near(b)

        @pl.when(b == 0)
        def _():
            forward(pairs - 1)

    loop(0, blocks, last_steps)
    project_far(pairs - 2)

    def finish(b):
        out[pl.ds(pl.multiple_of(b * rows, rows), rows), :] = acc[b].astype(BF16)

    loop(0, blocks, finish)

    def sent_asks(s):
        ask_copy(s, me).wait_send()
        for c in range(CAP):
            q_copy(s, me, c).wait_send()

    loop(0, me, sent_asks)

    def sent_results(r):
        for c in range(CAP):
            o_copy(r, me, c).wait_send()
            l_copy(r, me, c).wait_send()

    loop(me + 1, n_seq, sent_results)
    for d in range(1, n_head):
        order_copy(d).wait_send()

    def sent_heads(i):
        near_copy(i).wait_send()
        for step in range(1, n_x):
            cross_copy(step, i).wait_send()
            fwd_copy(step, i).wait_send()

    loop(0, pairs, sent_heads)


def solution(mesh):
    n_seq, n_head = mesh.shape["seq"], mesh.shape["head"]

    def body(query_rows, key_rows, value_rows, block_picks, out_weight):
        tok_rows, feature_width = query_rows.shape
        blocks, heads, n_pick = block_picks.shape
        rows, width = tok_rows // blocks, feature_width // heads
        pairs = blocks * heads
        crossings = max(n_head // 2 - 1, 1)
        any_spec = pl.BlockSpec(memory_space=pl.ANY)
        smem_spec = pl.BlockSpec(memory_space=pltpu.SMEM)
        vmem_spec = pl.BlockSpec(memory_space=pltpu.VMEM)
        out_width = out_weight.shape[1]
        slots = n_seq * CAP
        dma = pltpu.SemaphoreType.DMA
        dims = (n_seq, n_head, blocks, heads, n_pick, rows, width)
        tiles = pltpu.VMEM((pairs, rows, width), BF16)
        return pl.pallas_call(
            functools.partial(kernel, dims),
            out_shape=jax.ShapeDtypeStruct((tok_rows, out_width), BF16),
            in_specs=[any_spec] * 3 + [smem_spec] + [any_spec],
            out_specs=vmem_spec,
            scratch_shapes=[
                tiles,
                tiles,
                tiles,
                pltpu.VMEM((out_weight.shape[0] // width, width, out_width), BF16),
                pltpu.SMEM((pairs * n_pick,), jnp.int32),
                pltpu.SMEM((n_seq,), jnp.int32),
                pltpu.SMEM((pairs * n_pick,), jnp.int32),
                pltpu.SMEM((n_seq, CAP), jnp.int32),
                pltpu.SMEM((n_seq, CAP), jnp.int32),
                pltpu.SMEM((n_seq, CAP), jnp.int32),
                pltpu.SMEM((2, pairs), jnp.int32),
                pltpu.SMEM((n_head, 2, pairs), jnp.int32),
                pltpu.VMEM((slots, rows, width), BF16),
                pltpu.VMEM((slots, rows, width), BF16),
                pltpu.VMEM((slots, width, rows), BF16),
                pltpu.VMEM((slots, width, rows), BF16),
                pltpu.VMEM((slots, 1, rows), F32),
                pltpu.VMEM((slots, 1, rows), F32),
                pltpu.VMEM((slots, width, rows), BF16),
                pltpu.VMEM((slots, 1, rows), F32),
                tiles,
                tiles,
                pltpu.VMEM((crossings, pairs, rows, width), BF16),
                pltpu.VMEM((crossings, pairs, rows, width), BF16),
                pltpu.VMEM((blocks, rows, out_width), F32),
                dma((3, pairs)),
                dma((1,)),
                dma((2, n_seq)),
                dma((2, n_head)),
                dma((2, slots)),
                dma((2, slots)),
                dma((2, slots)),
                dma((2, pairs)),
                dma((2, crossings, pairs)),
                dma((2, crossings, pairs)),
            ],
            compiler_params=pltpu.CompilerParams(
                collective_id=0,
                has_side_effects=True,
                vmem_limit_bytes=67043328,
            ),
            name="layer",
        )(query_rows, key_rows, value_rows, jnp.swapaxes(block_picks, 1, 2),
          out_weight.reshape(-1, width, out_width))

    return jax.shard_map(
        body,
        mesh=mesh,
        in_specs=(
            P("seq", "head"),
            P("seq", "head"),
            P("seq", "head"),
            P("seq", "head", None),
            P(None, "head"),
        ),
        out_specs=P("seq", "head"),
        check_vma=False,
    )
```
